32 devices in a mesh: seqa: 8 (over z, x), seqb: 4 (over y, core).
Axes of the slice: x: 2, y: 2, z: 4, core: 2. Of those that a mesh axis runs over, the one named last changes fastest.
Arguments:
- queries: bfloat16 [16384, 4096], P(('seqa', 'seqb')), may hold values from -60 to 60
- keys: bfloat16 [16384, 1024], P(('seqa', 'seqb')), may hold values from -8 to 8
- values: bfloat16 [16384, 1024], P(('seqa', 'seqb')), may hold values from -6 to 6
- doc_start: int32 [16384], P(('seqa', 'seqb')), may hold values from 0 to 16383, as said below
Outputs:
- attended: bfloat16 [16384, 4096], P(('seqa', 'seqb'))
The draws below stay inside these ranges and needn't reach their ends.
Inputs may be any that keep to these rules, and one draw needn't show every extreme that they name: Never falling along the sequence, doc_start[i] <= i, the same value for all tokens of one document, and doc_start[0] = 0.
All inputs are finite; a program needn't handle non-finite values.
Results may differ from the reference program's by a relative error of at most 0.0038.
Values may be sent and summed in bfloat16 or wider, within the bound.
A program may use at most 64 MiB of HBM per device.

```python
import math
import jax
import jax.numpy as jnp
from jax import lax

QUERY_HEADS = 32
KEY_VALUE_HEADS = 8
HEAD_SIZE = 128
TOK_DEV = 512
SEQUENCE_TOKENS = 16384


def query_key_pair(key):
    base = jax.random.fold_in(key, 11)
    query_key, key_random_seed = jax.random.split(base, 2)
    sampled_keys = jax.random.truncated_normal(key_random_seed, -6.0, 6.0, (SEQUENCE_TOKENS, KEY_VALUE_HEADS * HEAD_SIZE), jnp.float32)
    queries_drawn = jax.random.truncated_normal(query_key, -6.0, 6.0, (SEQUENCE_TOKENS, QUERY_HEADS * HEAD_SIZE), jnp.float32)
    return (queries_drawn, sampled_keys)


def draw_queries(key, part):
    return query_key_pair(key)[0].astype(jnp.bfloat16)


def draw_keys(key, part):
    return query_key_pair(key)[1].astype(jnp.bfloat16)


def draw_doc_start(key, part):
    marks = jax.random.randint(jax.random.fold_in(key, 3), (SEQUENCE_TOKENS,), 0, 2 * TOK_DEV)
    places = jnp.arange(SEQUENCE_TOKENS, dtype=jnp.int32)
    opening = (marks == 0) & (places >= 3 * TOK_DEV) | (places == 0)
    begins = jnp.where(opening, places, 0).astype(jnp.int32)
    return lax.cummax(begins, axis=0)


def shard_levels(own_key, shape, cuts, smallest, largest):
    def one(axis_at, parts):
        heights = jax.random.uniform(jax.random.fold_in(jax.random.fold_in(own_key, 6), axis_at), (parts,), jnp.float32, smallest / len(cuts), largest / len(cuts))
        return jnp.repeat(jnp.exp(heights), shape[axis_at] // parts).reshape((-1,) + (1,) * (len(shape) - axis_at - 1))

    gain = one(*cuts[0])
    for cut in cuts[1:]:
        gain = gain * one(*cut)
    return gain


def scatter_about(rng, shape, width, limit, shards=(), kind=jnp.bfloat16):
    loudness = shard_levels(rng, shape, shards, -0.22, 0.18) if shards else 1.0
    values = jax.random.normal(rng, shape, jnp.float32) * width * loudness
    return jnp.minimum(jnp.maximum(values, -limit), limit).astype(kind)


def setup_inputs(seed: int = 0) -> dict:
    arg_keys = jax.random.split(jax.random.key(seed), 5)
    queries = draw_queries(jax.random.fold_in(arg_keys[4], 71), 0)
    keys = draw_keys(jax.random.fold_in(arg_keys[4], 71), 0)
    values = scatter_about(arg_keys[2], (SEQUENCE_TOKENS, KEY_VALUE_HEADS * HEAD_SIZE), 1.0, 6.0, ((0, 32),))
    doc_start = draw_doc_start(jax.random.fold_in(arg_keys[4], 71), 0)
    return {"queries": queries, "keys": keys, "values": values, "doc_start": doc_start}


def reference(queries, keys, values, doc_start):
    rows_per_block = min(512, TOK_DEV)
    window_length = 2 * TOK_DEV
    group_width = QUERY_HEADS // KEY_VALUE_HEADS
    score_scale = 1.0 / math.sqrt(HEAD_SIZE)
    padded_keys = jnp.concatenate([jnp.zeros((window_length, KEY_VALUE_HEADS * HEAD_SIZE), jnp.bfloat16), keys], axis=0)
    padded_values = jnp.concatenate([jnp.zeros((window_length, KEY_VALUE_HEADS * HEAD_SIZE), jnp.bfloat16), values], axis=0)

    def one_block(block_index):
        offset = (block_index * rows_per_block).astype(jnp.int32)
        block_of_queries = lax.dynamic_slice_in_dim(queries, offset, rows_per_block, 0).astype(jnp.float32)
        block_of_queries = block_of_queries.reshape(rows_per_block, KEY_VALUE_HEADS, group_width, HEAD_SIZE)
        block_of_keys = lax.dynamic_slice_in_dim(padded_keys, offset, window_length + rows_per_block, 0).astype(jnp.float32)
        block_of_keys = block_of_keys.reshape(window_length + rows_per_block, KEY_VALUE_HEADS, HEAD_SIZE)
        block_of_values = lax.dynamic_slice_in_dim(padded_values, offset, window_length + rows_per_block, 0).astype(jnp.float32)
        block_of_values = block_of_values.reshape(window_length + rows_per_block, KEY_VALUE_HEADS, HEAD_SIZE)
        scores = jnp.einsum('thgd,khd->hgtk', block_of_queries, block_of_keys) * score_scale
        query_place = offset + jnp.arange(rows_per_block, dtype=jnp.int32)
        key_place = offset - window_length + jnp.arange(window_length + rows_per_block, dtype=jnp.int32)
        starts = lax.dynamic_slice_in_dim(doc_start, offset, rows_per_block, 0)
        visible = (key_place[None, :] <= query_place[:, None]) & (key_place[None, :] > query_place[:, None] - window_length) & (key_place[None, :] >= starts[:, None])
        scores = jnp.where(visible[None, None], scores, jnp.float32(-1e+30))
        row_top = lax.optimization_barrier(jnp.max(scores, axis=-1, keepdims=True))
        exponent = jnp.where(visible[None, None], jnp.exp(scores - row_top), jnp.float32(0.0))
        row_sum = lax.optimization_barrier(jnp.sum(exponent, axis=-1, keepdims=True))
        weights = exponent.astype(jnp.bfloat16).astype(jnp.float32)
        summed = jnp.einsum('hgtk,khd->thgd', weights, block_of_values)
        result = summed / jnp.transpose(row_sum, (2, 0, 1, 3))
        return result.reshape(rows_per_block, QUERY_HEADS * HEAD_SIZE).astype(jnp.bfloat16)
    blocks = lax.map(one_block, jnp.arange(SEQUENCE_TOKENS // rows_per_block, dtype=jnp.int32))
    return blocks.reshape(SEQUENCE_TOKENS, QUERY_HEADS * HEAD_SIZE)
```

```python
import functools
import math

import jax
import jax.numpy as jnp
from jax import lax
from jax.experimental import pallas as pl
from jax.experimental.pallas import tpu as pltpu
from jax.sharding import PartitionSpec as P

HEAD_SIZE = 128
AXES = ("seqa", "seqb")
MESH = pl.DeviceIdType.MESH
HIDDEN = -1e30


def kernel(
    sizes,
    starts_ref,
    queries_ref,
    keys_ref,
    values_ref,
    keys_hbm,
    values_hbm,
    out_ref,
    received,
    values_t,
    scores,
    weights,
    key_marks,
    query_marks,
    edge_bias,
    diag_bias,
    send_sem,
    recv_sem,
):
    across, inner, heads, group, rows, block = sizes
    devices = across * inner
    head = HEAD_SIZE
    blocks = rows // block
    tiles = 2 * blocks + 1
    step = pl.program_id(0)
    me = lax.axis_index("seqa") * inner + lax.axis_index("seqb")
    parity = lax.rem(me, 2)

    def place(shift):
        target = lax.rem(me + shift + devices, devices)
        return (target // inner, lax.rem(target, inner))

    def send(which, kind, h, source, target):
        return pltpu.make_async_remote_copy(
            src_ref=source,
            dst_ref=received.at[kind, h, pl.ds(which * rows, rows), :],
            send_sem=send_sem.at[which, kind, h],
            recv_sem=recv_sem.at[which, kind, h],
            device_id=target,
            device_id_type=MESH,
        )

    def own(kind, h):
        ref = values_hbm if kind else keys_hbm
        return ref.at[:, pl.ds(pl.multiple_of(h * head, head), head)]

    def landed(which, kind, h):
        return received.at[kind, h, pl.ds(which * rows, rows), :]

    @pl.when(step == 0)
    def _():
        barrier = pltpu.get_barrier_semaphore()
        for shift in (-2, -1, 1, 2):
            pl.semaphore_signal(barrier, inc=1, device_id=place(shift), device_id_type=MESH)
        pl.semaphore_wait(barrier, 4)

        def start_all(h, carry):
            for kind in range(2):
                send(0, kind, h, own(kind, h), place(2)).start()

            @pl.when(parity == 0)
            def _():
                for kind in range(2):
                    send(1, kind, h, own(kind, h), place(1)).start()

            return carry

        lax.fori_loop(0, heads, start_all, 0)

        key_at = lax.broadcasted_iota(jnp.int32, (block, block), 0)
        query_at = lax.broadcasted_iota(jnp.int32, (block, block), 1)
        edge_bias[...] = jnp.where(key_at > query_at, 0.0, HIDDEN)
        lane = lax.broadcasted_iota(jnp.int32, (block, head), 1)
        row = lax.broadcasted_iota(jnp.int32, (block, head), 0)
        for b in range(blocks):
            base = me * rows + b * block
            start = starts_ref[0:1, b * block : (b + 1) * block]
            diag_bias[b] = jnp.where(
                (key_at <= query_at) & (key_at + base >= start), 0.0, HIDDEN
            )
            first = jnp.broadcast_to(start[:, 0:1], (block, head))
            other = jnp.broadcast_to(jnp.where(start > base, 1.0, 0.0), (head, block)).T
            marks = jnp.where(lane == 0, 1.0, jnp.where(lane == 1, other, 0.0)) * HIDDEN
            query_marks[b] = marks.astype(jnp.bfloat16)
            for t in range(tiles - 1):
                at = row + (base - 2 * rows + t * block)
                before = jnp.where(at < first, 1.0, 0.0)
                mark = jnp.where(lane == 0, before, jnp.where(lane == 1, 1.0, 0.0))
                key_marks[b, t] = mark.astype(jnp.bfloat16)
            key_marks[b, tiles - 1] = jnp.zeros((block, head), jnp.bfloat16)

    for kind in range(2):
        send(0, kind, step, own(kind, step), place(2)).wait_recv()

    @pl.when(parity == 1)
    def _():
        for kind in range(2):
            send(1, kind, step, landed(0, kind, step), place(-1)).start()

    for kind in range(2):
        send(1, kind, step, own(kind, step), place(1)).wait_recv()

    for b in range(2 * blocks):
        part = received[1, step, b * block : (b + 1) * block, :]
        values_t[:, b * block : (b + 1) * block] = part.T
    for b in range(blocks):
        part = values_ref[b * block : (b + 1) * block, :]
        values_t[:, (2 * blocks + b) * block : (2 * blocks + b + 1) * block] = part.T

    scale = math.log2(math.e) / math.sqrt(head)
    units = [(g, b) for b in range(blocks) for g in range(group)]

    def query_side(u):
        g, b = units[u]
        q = queries_ref[b * block : (b + 1) * block, g * head : (g + 1) * head]
        q = (q.astype(jnp.float32) * scale).astype(jnp.bfloat16)
        return jnp.concatenate([q, query_marks[b]], axis=1)

    def score_tile(u, t, q, top):
        g, b = units[u]
        at = b + t
        if at < 2 * blocks:
            k = received[0, step, at * block : (at + 1) * block, :]
        else:
            k = keys_ref[(at - 2 * blocks) * block : (at - 2 * blocks + 1) * block, :]
        k = jnp.concatenate([k, key_marks[b, t]], axis=1)
        s = lax.dot_general(k, q, (((1,), (1,)), ((), ())), preferred_element_type=jnp.float32)
        if t == 0:
            s = s + edge_bias[...]
        if t == tiles - 1:
            s = s + diag_bias[b]
        scores[u % 2, t * block : (t + 1) * block, :] = s
        partial = jnp.max(s.reshape(block // 8, 8, block), axis=0)
        return partial if top is None else jnp.maximum(top, partial)

    def weigh_tile(u, t, top, total):
        s = scores[u % 2, t * block : (t + 1) * block, :]
        p = jnp.exp2(s - top)
        weights[u % 2, t * block : (t + 1) * block, :] = p.astype(jnp.bfloat16)
        partial = jnp.sum(p.reshape(block // 8, 8, block), axis=0)
        return partial if total is None else total + partial

    def finish(u, total):
        g, b = units[u]
        v = values_t[:, b * block : (b + tiles) * block]
        summed = jnp.dot(v, weights[u % 2], preferred_element_type=jnp.float32)
        summed = summed / jnp.sum(total, axis=0, keepdims=True)
        out_ref[b * block : (b + 1) * block, g * head : (g + 1) * head] = summed.T.astype(
            jnp.bfloat16
        )

    top = None
    q = query_side(0)
    for t in range(tiles):
        top = score_tile(0, t, q, top)
    for u in range(len(units)):
        top_now = jnp.max(top, axis=0, keepdims=True)
        top, total = None, None
        last = u == len(units) - 1
        if not last:
            q = query_side(u + 1)
        for t in range(tiles):
            if not last:
                top = score_tile(u + 1, t, q, top)
            total = weigh_tile(u, t, top_now, total)
        finish(u, total)

    @pl.when(step == heads - 1)
    def _():
        def end_all(h, carry):
            for which in range(2):
                for kind in range(2):
                    send(which, kind, h, own(kind, h), place(2)).wait_send()
            return carry

        lax.fori_loop(0, heads, end_all, 0)


def local(mesh, queries, keys, values, doc_start):
    rows = queries.shape[0]
    head = HEAD_SIZE
    heads = keys.shape[1] // head
    group = queries.shape[1] // keys.shape[1]
    block = rows // 2
    blocks = rows // block
    tiles = 2 * blocks + 1
    sizes = (mesh.shape["seqa"], mesh.shape["seqb"], heads, group, rows, block)
    assert (sizes[0] * sizes[1]) % 2 == 0
    return pl.pallas_call(
        functools.partial(kernel, sizes),
        grid=(heads,),
        out_shape=jax.ShapeDtypeStruct(queries.shape, jnp.bfloat16),
        in_specs=[
            pl.BlockSpec((1, rows), lambda h: (0, 0)),
            pl.BlockSpec((rows, group * head), lambda h: (0, h)),
            pl.BlockSpec((rows, head), lambda h: (0, h)),
            pl.BlockSpec((rows, head), lambda h: (0, h)),
            pl.BlockSpec(memory_space=pl.ANY),
            pl.BlockSpec(memory_space=pl.ANY),
        ],
        out_specs=pl.BlockSpec((rows, group * head), lambda h: (0, h)),
        scratch_shapes=[
            pltpu.VMEM((2, heads, 2 * rows, head), jnp.bfloat16),
            pltpu.VMEM((head, 3 * rows), jnp.bfloat16),
            pltpu.VMEM((2, tiles * block, block), jnp.float32),
            pltpu.VMEM((2, tiles * block, block), jnp.bfloat16),
            pltpu.VMEM((blocks, tiles, block, head), jnp.bfloat16),
            pltpu.VMEM((blocks, block, head), jnp.bfloat16),
            pltpu.VMEM((block, block), jnp.float32),
            pltpu.VMEM((blocks, block, block), jnp.float32),
            pltpu.SemaphoreType.DMA((2, 2, heads)),
            pltpu.SemaphoreType.DMA((2, 2, heads)),
        ],
        compiler_params=pltpu.CompilerParams(
            collective_id=0,
            has_side_effects=True,
            dimension_semantics=("arbitrary",),
            vmem_limit_bytes=60 * 1024 * 1024,
        ),
    )(doc_start.reshape(1, rows), queries, keys, values, keys, values)


def solution(mesh):
    return jax.shard_map(
        functools.partial(local, mesh),
        mesh=mesh,
        in_specs=(P(AXES, None), P(AXES, None), P(AXES, None), P(AXES)),
        out_specs=P(AXES, None),
        check_vma=False,
    )
```

```python
import functools
import math

import jax
import jax.numpy as jnp
from jax import lax
from jax.experimental import pallas as pl
from jax.experimental.pallas import tpu as pltpu
from jax.sharding import PartitionSpec as P

HEAD_SIZE = 128
AXES = ("seqa", "seqb")
MESH = pl.DeviceIdType.MESH
HIDDEN = -1e30


def kernel(
    sizes,
    starts_ref,
    queries_hbm,
    keys_hbm,
    values_hbm,
    out_ref,
    received,
    values_t,
    scores,
    weights,
    key_marks,
    query_marks,
    edge_bias,
    diag_bias,
    queries_in,
    keys_in,
    values_in,
    send_sem,
    recv_sem,
    fetch_sem,
):
    across, inner, heads, group, rows, block = sizes
    devices = across * inner
    head = HEAD_SIZE
    blocks = rows // block
    tiles = 2 * blocks + 1
    step = pl.program_id(0)
    me = lax.axis_index("seqa") * inner + lax.axis_index("seqb")
    parity = lax.rem(me, 2)

    def place(shift):
        target = lax.rem(me + shift + devices, devices)
        return (target // inner, lax.rem(target, inner))

    def send(which, kind, h, source, target):
        return pltpu.make_async_remote_copy(
            src_ref=source,
            dst_ref=received.at[kind, h, pl.ds(which * rows, rows), :],
            send_sem=send_sem.at[which, kind, h],
            recv_sem=recv_sem.at[which, kind, h],
            device_id=target,
            device_id_type=MESH,
        )

    def own(kind, h):
        ref = values_hbm if kind else keys_hbm
        return ref.at[:, pl.ds(pl.multiple_of(h * head, head), head)]

    def landed(which, kind, h):
        return received.at[kind, h, pl.ds(which * rows, rows), :]

    has = {0: me >= 2, 1: me >= 1}
    feeds = {0: me + 2 < devices, 1: jnp.where(parity == 0, me + 1 < devices, me >= 2)}

    def fetch(h):
        at = pl.ds(pl.multiple_of(h * head, head), head)
        wide = pl.ds(pl.multiple_of(h * group * head, group * head), group * head)
        return (
            pltpu.make_async_copy(queries_hbm.at[:, wide], queries_in.at[h], fetch_sem.at[0, h]),
            pltpu.make_async_copy(keys_hbm.at[:, at], keys_in.at[h], fetch_sem.at[1, h]),
            pltpu.make_async_copy(values_hbm.at[:, at], values_in.at[h], fetch_sem.at[2, h]),
        )

    @pl.when(step == 0)
    def _():
        barrier = pltpu.get_barrier_semaphore()
        near = ((-2, me >= 2), (-1, me >= 1), (1, me + 1 < devices), (2, me + 2 < devices))
        for shift, there in near:

            @pl.when(there)
            def _():
                pl.semaphore_signal(barrier, inc=1, device_id=place(shift), device_id_type=MESH)

        count = sum(there.astype(jnp.int32) for _, there in near)
        pl.semaphore_wait(barrier, count)

        def start_all(h, carry):
            for kind in range(2):

                @pl.when(feeds[0])
                def _():
                    send(0, kind, h, own(kind, h), place(2)).start()

                @pl.when((parity == 0) & feeds[1])
                def _():
                    send(1, kind, h, own(kind, h), place(1)).start()

            return carry

        lax.fori_loop(0, heads, start_all, 0)

        def fetch_all(h, carry):
            for copy in fetch(h):
                copy.start()
            return carry

        lax.fori_loop(0, heads, fetch_all, 0)

        for which in range(2):

            @pl.when(jnp.logical_not(has[which]))
            def _():
                for kind in range(2):
                    for h in range(heads):
                        received[kind, h, which * rows : (which + 1) * rows, :] = jnp.zeros(
                            (rows, head), jnp.bfloat16
                        )

        key_at = lax.broadcasted_iota(jnp.int32, (block, block), 0)
        query_at = lax.broadcasted_iota(jnp.int32, (block, block), 1)
        edge_bias[...] = jnp.where(key_at > query_at, 0.0, HIDDEN)
        lane = lax.broadcasted_iota(jnp.int32, (block, head), 1)
        row = lax.broadcasted_iota(jnp.int32, (block, head), 0)
        for b in range(blocks):
            base = me * rows + b * block
            start = starts_ref[0:1, b * block : (b + 1) * block]
            diag_bias[b] = jnp.where(
                (key_at <= query_at) & (key_at + base >= start), 0.0, HIDDEN
            )
            first = jnp.broadcast_to(start[:, 0:1], (block, head))
            other = jnp.broadcast_to(jnp.where(start > base, 1.0, 0.0), (head, block)).T
            marks = jnp.where(lane == 0, 1.0, jnp.where(lane == 1, other, 0.0)) * HIDDEN
            query_marks[b] = marks.astype(jnp.bfloat16)
            for t in range(tiles - 1):
                at = row + (base - 2 * rows + t * block)
                before = jnp.where(at < first, 1.0, 0.0)
                mark = jnp.where(lane == 0, before, jnp.where(lane == 1, 1.0, 0.0))
                key_marks[b, t] = mark.astype(jnp.bfloat16)
            key_marks[b, tiles - 1] = jnp.zeros((block, head), jnp.bfloat16)

    def arrive(kind):
        @pl.when(has[0])
        def _():
            send(0, kind, step, own(kind, step), place(2)).wait_recv()

        @pl.when((parity == 1) & has[0])
        def _():
            send(1, kind, step, landed(0, kind, step), place(-1)).start()

        @pl.when(has[1])
        def _():
            send(1, kind, step, own(kind, step), place(1)).wait_recv()

    for copy in fetch(step):
        copy.wait()
    arrive(0)

    scale = math.log2(math.e) / math.sqrt(head)
    units = [(g, b) for b in range(blocks) for g in range(group)]

    def query_side(u):
        g, b = units[u]
        q = queries_in[step, b * block : (b + 1) * block, g * head : (g + 1) * head]
        q = (q.astype(jnp.float32) * scale).astype(jnp.bfloat16)
        return jnp.concatenate([q, query_marks[b]], axis=1)

    def score_tile(u, t, q, top):
        g, b = units[u]
        at = b + t
        if at < 2 * blocks:
            k = received[0, step, at * block : (at + 1) * block, :]
        else:
            k = keys_in[step, (at - 2 * blocks) * block : (at - 2 * blocks + 1) * block, :]
        k = jnp.concatenate([k, key_marks[b, t]], axis=1)
        s = lax.dot_general(k, q, (((1,), (1,)), ((), ())), preferred_element_type=jnp.float32)
        if t == 0:
            s = s + edge_bias[...]
        if t == tiles - 1:
            s = s + diag_bias[b]
        scores[u % 2, t * block : (t + 1) * block, :] = s
        partial = jnp.max(s.reshape(block // 8, 8, block), axis=0)
        return partial if top is None else jnp.maximum(top, partial)

    def weigh_tile(u, t, top, total):
        s = scores[u % 2, t * block : (t + 1) * block, :]
        p = jnp.exp2(s - top)
        weights[u, t * block : (t + 1) * block, :] = p.astype(jnp.bfloat16)
        partial = jnp.sum(p.reshape(block // 8, 8, block), axis=0)
        return partial if total is None else total + partial

    def finish(u, total):
        g, b = units[u]
        v = values_t[:, b * block : (b + tiles) * block]
        summed = jnp.dot(v, weights[u], preferred_element_type=jnp.float32)
        summed = summed * total
        at = pl.ds(pl.multiple_of((step * group + g) * head, head), head)
        out_ref[b * block : (b + 1) * block, at] = summed.T.astype(jnp.bfloat16)

    totals = []
    top = None
    q = query_side(0)
    for t in range(tiles):
        top = score_tile(0, t, q, top)
    for u in range(len(units)):
        top_now = jnp.max(top, axis=0, keepdims=True)
        top, total = None, None
        last = u == len(units) - 1
        if not last:
            q = query_side(u + 1)
        for t in range(tiles):
            if not last:
                top = score_tile(u + 1, t, q, top)
            total = weigh_tile(u, t, top_now, total)
        totals.append(1.0 / jnp.sum(total, axis=0, keepdims=True))

    arrive(1)
    for b in range(3 * blocks):
        if b < 2 * blocks:
            part = received[1, step, b * block : (b + 1) * block, :]
        else:
            part = values_in[step, (b - 2 * blocks) * block : (b - 2 * blocks + 1) * block, :]
        values_t[:, b * block : (b + 1) * block] = part.T
    for u in range(len(units)):
        finish(u, totals[u])

    @pl.when(step == heads - 1)
    def _():
        def end_all(h, carry):
            for which in range(2):

                @pl.when(feeds[which])
                def _():
                    for kind in range(2):
                        send(which, kind, h, own(kind, h), place(1)).wait_send()

            return carry

        lax.fori_loop(0, heads, end_all, 0)


def local(mesh, queries, keys, values, doc_start):
    rows = queries.shape[0]
    head = HEAD_SIZE
    heads = keys.shape[1] // head
    group = queries.shape[1] // keys.shape[1]
    block = rows // 2
    blocks = rows // block
    tiles = 2 * blocks + 1
    sizes = (mesh.shape["seqa"], mesh.shape["seqb"], heads, group, rows, block)
    assert (sizes[0] * sizes[1]) % 2 == 0
    return pl.pallas_call(
        functools.partial(kernel, sizes),
        grid=(heads,),
        out_shape=pltpu.VMEM(queries.shape, jnp.bfloat16),
        in_specs=[
            pl.BlockSpec((1, rows), lambda h: (0, 0)),
            pl.BlockSpec(memory_space=pl.ANY),
            pl.BlockSpec(memory_space=pl.ANY),
            pl.BlockSpec(memory_space=pl.ANY),
        ],
        out_specs=pl.BlockSpec(memory_space=pltpu.VMEM),
        scratch_shapes=[
            pltpu.VMEM((2, heads, 2 * rows, head), jnp.bfloat16),
            pltpu.VMEM((head, 3 * rows), jnp.bfloat16),
            pltpu.VMEM((2, tiles * block, block), jnp.float32),
            pltpu.VMEM((group * blocks, tiles * block, block), jnp.bfloat16),
            pltpu.VMEM((blocks, tiles, block, head), jnp.bfloat16),
            pltpu.VMEM((blocks, block, head), jnp.bfloat16),
            pltpu.VMEM((block, block), jnp.float32),
            pltpu.VMEM((blocks, block, block), jnp.float32),
            pltpu.VMEM((heads, rows, group * head), jnp.bfloat16),
            pltpu.VMEM((heads, rows, head), jnp.bfloat16),
            pltpu.VMEM((heads, rows, head), jnp.bfloat16),
            pltpu.SemaphoreType.DMA((2, 2, heads)),
            pltpu.SemaphoreType.DMA((2, 2, heads)),
            pltpu.SemaphoreType.DMA((3, heads)),
        ],
        compiler_params=pltpu.CompilerParams(
            collective_id=0,
            has_side_effects=True,
            dimension_semantics=("arbitrary",),
            vmem_limit_bytes=59 * 1024 * 1024,
        ),
    )(doc_start.reshape(1, rows), queries, keys, values)


def solution(mesh):
    return jax.shard_map(
        functools.partial(local, mesh),
        mesh=mesh,
        in_specs=(P(AXES, None), P(AXES, None), P(AXES, None), P(AXES)),
        out_specs=P(AXES, None),
        check_vma=False,
    )
```
